32 devices in a mesh: field: 2 (over x), ep: 16 (over z, y, core).
Axes of the slice: x: 2, y: 2, z: 4, core: 2. Of those that a mesh axis runs over, the one named last changes fastest.
Arguments:
- images: float32 [64, 16, 256], P(('field', 'ep')), parts along dimension 0, may hold values from -6 to 6
- reference_image: float32 [32, 256], P('field'), parts along dimension 0, may hold values from -6 to 6
- kernels: float32 [16, 23, 23], replicated, may hold values from -0.25 to 0.25
- kernel_index: int32 [64], P(('field', 'ep')), parts along dimension 0, may hold values from 0 to 15
- tile_mask: int32 [64, 16, 2], P(('field', 'ep')), parts along dimension 0, may hold values 0 or 1
- systematics: float32 [64, 40], P('field'), parts along dimension 0, may hold values from -6 to 6
- onsets: int32 [16], P('field'), parts along dimension 0, may hold values from 0 to 27
Outputs:
- coefficients: float32 [48, 32, 256], P(None, ('field', 'ep')), parts along dimension 1
- epoch_scatter: float32 [64], P('field'), parts along dimension 0
The draws below stay inside these ranges and needn't reach their ends.
There are 2 independent parts, one for each index of `field`. The reference program is written for one: setup_inputs(seed, part) draws one part's arguments, and reference() takes and returns one part's arrays. A program takes and returns all parts, laid end to end along the dimension named above; an argument that names none is the same for every part. Nothing has to cross between parts.
All inputs are finite; a program needn't handle non-finite values. No bound on the sum of `tile_mask` on one device may be relied on, other than what follows from the above.
Results may differ from the reference program's by a relative error of at most 0.00011.
Values sent between devices are 32-bit elements; how exact they have to be, the bound alone decides.
A program may use at most 64 MiB of HBM per device.

```python
import jax
import jax.numpy as jnp
from jax import lax

W = 256
KS = 23
NK = 16
NSYS = 40
NTR = 8
R = 16
E = 32


def touch_ends(drawn, stream_key, smallest, high):
    dims = drawn.shape
    spot = [jax.random.randint(jax.random.fold_in(stream_key, axis), (), 0, dims[axis]) for axis in range(len(dims))]
    drawn = drawn.at[tuple(spot)].set(smallest)
    longest = dims.index(max(dims))
    spot[longest] = (spot[longest] + 1) % dims[longest]
    return drawn.at[tuple(spot)].set(high)


def block_levels(rng, dims, cuts, least, largest):
    level, own = 1.0, jax.random.fold_in(rng, 6)
    for position, shards_of in cuts:
        steps = jnp.exp(jax.random.uniform(jax.random.fold_in(own, position), (shards_of,), jnp.float32, least / len(cuts), largest / len(cuts)))
        level = level * jnp.repeat(steps, dims[position] // shards_of).reshape([-1 if axis == position else 1 for axis in range(len(dims))])
    return level


def noise(stream_key, dims, scale, reach, shards=(), kind=jnp.bfloat16):
    factor_of = block_levels(stream_key, dims, shards, -0.22, 0.18) if shards else 1.0
    values = jax.random.normal(stream_key, dims, jnp.float32) * scale * factor_of
    return jnp.minimum(jnp.maximum(values, -reach), reach).astype(kind)


def setup_inputs(seed: int = 0, part: int = 0) -> dict:
    splits = jax.random.split(jax.random.key(seed), 8)
    own_keys = jax.random.split(jax.random.fold_in(splits[7], part), 8)
    images = noise(own_keys[0], (E, R, W), 1.0, 6.0, ((0, 16),), jnp.float32)
    reference_image = noise(own_keys[1], (R, W), 1.0, 6.0, (), jnp.float32)
    kernels = noise(splits[2], (NK, KS, KS), (KS * KS) ** -0.5, 0.25, (), jnp.float32)
    kernel_index = touch_ends(jax.random.randint(own_keys[3], (E,), 0, NK), jax.random.fold_in(own_keys[3], 1), 0, NK - 1).astype(jnp.int32)
    tile_mask = touch_ends((jax.random.randint(own_keys[4], (E, R, W // 128), 0, 8) < 7).astype(jnp.int32), jax.random.fold_in(own_keys[4], 1), 0, 1)
    systematics = noise(own_keys[5], (E, NSYS), 1.0, 6.0, (), jnp.float32)
    onsets = touch_ends(jax.random.randint(own_keys[6], (NTR,), 0, E - 4), jax.random.fold_in(own_keys[6], 1), 0, (E - 4) - 1).astype(jnp.int32)
    return dict(images=images, reference_image=reference_image, kernels=kernels, kernel_index=kernel_index, tile_mask=tile_mask, systematics=systematics, onsets=onsets)


cov_ridge = 0.5
fit_ridge = 1.0

def correlate(stack, chosen):
    count = stack.shape[0]
    filters = jnp.transpose(chosen, (1, 2, 0))[:, :, None, :]
    result = lax.conv_general_dilated(stack[None], filters, (1, 1), 'SAME', dimension_numbers=('NCHW', 'HWIO', 'NCHW'), feature_group_count=count, precision=lax.Precision.HIGHEST)
    return result[0]

def subtract(stack, reference_image, chosen, masks):
    result = reference_image[None] - correlate(stack, chosen)
    shape = result.shape
    tiles = result.reshape(shape[0], shape[1], shape[2] // 128, 128) * masks[..., None].astype(jnp.float32)
    return tiles.reshape(shape)

def build_design(systematics, onsets):
    count = systematics.shape[0]
    templates = onsets.shape[0]
    epoch_axis = jnp.arange(count, dtype=jnp.float32)[:, None]
    delays = epoch_axis - onsets[None, :].astype(jnp.float32)
    timescale = (jnp.arange(templates, dtype=jnp.float32) + 1.0) * count / (2.0 * templates)
    transient = jnp.where(delays >= 0.0, jnp.exp(-jnp.maximum(delays, 0.0) / timescale[None, :]), 0.0)
    return jnp.concatenate([systematics, transient.astype(systematics.dtype)], axis=1)

def fit_matrix(scatter, npixels, design):
    count = design.shape[0]
    columns = design.shape[1]
    covariance = scatter / npixels + cov_ridge * jnp.eye(count, dtype=scatter.dtype)
    lower = jnp.linalg.cholesky(covariance)
    weighted = jax.scipy.linalg.cho_solve((lower, True), design)
    normal = jnp.dot(design.T, weighted, precision=lax.Precision.HIGHEST) + fit_ridge * jnp.eye(columns, dtype=scatter.dtype)
    lower_fit = jnp.linalg.cholesky(normal)
    return jax.scipy.linalg.cho_solve((lower_fit, True), weighted.T)

def reference(images, reference_image, kernels, kernel_index, tile_mask, systematics, onsets):
    count, rows, width = images.shape
    chosen = kernels[kernel_index]
    difference = subtract(images, reference_image, chosen, tile_mask)
    pixel_data = difference.reshape(count, rows * width)
    scatter = jnp.dot(pixel_data, pixel_data.T, precision=lax.Precision.HIGHEST)
    npixels = float(rows * width)
    design = build_design(systematics, onsets)
    fit = fit_matrix(scatter, npixels, design)
    coefficients = jnp.dot(fit, pixel_data, precision=lax.Precision.HIGHEST)
    residual = pixel_data - jnp.dot(design, coefficients, precision=lax.Precision.HIGHEST)
    epoch_scatter = jnp.sum(residual * residual, axis=1) / npixels
    return (coefficients.reshape(design.shape[1], rows, width), epoch_scatter)
```

```python
import functools

import jax
import jax.numpy as jnp
from jax import lax
from jax.experimental import pallas as pl
from jax.experimental.pallas import tpu as pltpu
from jax.sharding import PartitionSpec as P

cov_ridge = 0.5
fit_ridge = 1.0
LANES = 128
HIGHEST = lax.Precision.HIGHEST


def dot(a, b, contract):
    return lax.dot_general(
        a, b, ((contract[0], contract[1]), ((), ())), precision=HIGHEST, preferred_element_type=jnp.float32
    )


def iota(shape, axis):
    return lax.broadcasted_iota(jnp.int32, shape, axis)


def kernel(
    n,
    images_ref,
    reference_ref,
    kernels_ref,
    index_ref,
    mask_ref,
    systematics_ref,
    onsets_ref,
    coefficients_ref,
    epoch_ref,
    table,
    table_t,
    taps,
    shifted,
    send,
    recv,
    pixels,
    part,
    parts,
    work,
    send_sem,
    recv_sem,
    part_send_sem,
    part_recv_sem,
):
    local, rows, width = images_ref.shape
    side = kernels_ref.shape[0]
    half = (side - 1) // 2
    tiles = width // LANES
    block = rows // n
    epochs = local * n
    nsys = systematics_ref.shape[1]
    ntr = onsets_ref.shape[0]
    columns = nsys + ntr
    npixels = float(rows * width)
    pack = max(LANES // epochs, 1)
    me = lax.axis_index("ep")

    barrier = pltpu.get_barrier_semaphore()
    for d in range(1, n):
        pl.semaphore_signal(
            barrier,
            inc=1,
            device_id={"ep": lax.rem(me + d, n)},
            device_id_type=pl.DeviceIdType.MESH,
        )

    depth = side * rows
    padded_depth = taps.shape[1]
    lane = iota((rows, LANES), 1)
    column = iota((rows, width), 1)
    for e in range(local):
        table[...] = jnp.zeros_like(table)
        for a in range(side):
            table[a : a + 1, 0:side] = kernels_ref[a, pl.ds(index_ref[e], 1), :]
        table[side + 1 : side + 1 + tiles, 0:rows] = mask_ref[e].astype(jnp.float32)
        table_t[...] = table[...].T
        kept = jnp.where(iota((side, LANES), 1) < side, table_t[0:side, :], 0.0)
        kept = pltpu.roll(kept, LANES - half, axis=1)
        groups = [jnp.zeros((rows, LANES), jnp.float32) for _ in range(padded_depth // LANES)]
        for b in range(side):
            start = b * rows
            at = start % LANES
            row = jnp.broadcast_to(kept[b : b + 1, :], (rows, LANES))
            turned = pltpu.roll(row, at, axis=1, stride=1, stride_axis=0)
            inside = (lane >= at) & (lane < at + rows)
            groups[start // LANES] = jnp.where(inside, turned, groups[start // LANES])
        for g, value in enumerate(groups):
            taps[:, g * LANES : (g + 1) * LANES] = value
        image = images_ref[e]
        for b in range(side):
            move = b - half
            moved = pltpu.roll(image, (-move) % width, axis=1) if move else image
            inside = (column + move >= 0) & (column + move < width)
            shifted[b * rows : (b + 1) * rows, :] = jnp.where(inside, moved, 0.0)
        if padded_depth > depth:
            shifted[depth:, :] = jnp.zeros((padded_depth - depth, width), jnp.float32)
        difference = reference_ref[...] - dot(taps[...], shifted[...], ((1,), (0,)))
        for t in range(tiles):
            good = table_t[0:rows, side + 1 + t : side + 2 + t]
            piece = difference[:, t * LANES : (t + 1) * LANES] * good
            for r in range(rows):
                slot = (r % block) * tiles * local + t * local + e
                send[r // block, slot : slot + 1, :] = piece[r : r + 1, :]

    pl.semaphore_wait(barrier, n - 1)

    def exchange(source, target, send_sems, recv_sems, d):
        return pltpu.make_async_remote_copy(
            src_ref=source,
            dst_ref=target,
            send_sem=send_sems.at[d],
            recv_sem=recv_sems.at[d],
            device_id={"ep": lax.rem(me + d, n)},
            device_id_type=pl.DeviceIdType.MESH,
        )

    for d in range(1, n):
        exchange(send.at[lax.rem(me + d, n)], recv.at[me], send_sem, recv_sem, d).start()
    recv[me] = send[me]

    work[...] = jnp.zeros_like(work)
    epoch = iota((epochs, LANES), 0).astype(jnp.float32)
    template = iota((epochs, LANES), 1)
    onset = jnp.zeros((epochs, LANES), jnp.float32)
    for k in range(ntr):
        onset = jnp.where(template == k, onsets_ref[k].astype(jnp.float32), onset)
    delays = epoch - onset
    timescale = (template.astype(jnp.float32) + 1.0) * epochs / (2.0 * ntr)
    transient = jnp.where(delays >= 0.0, jnp.exp(-jnp.maximum(delays, 0.0) / timescale), 0.0)
    work[:, epochs : epochs + nsys] = systematics_ref[...]
    work[:, epochs + nsys : epochs + columns] = transient[:, 0:ntr]
    design = work[...]
    outer = dot(design, design, ((1,), (1,)))

    for d in range(1, n):
        source = lax.rem(me - d + n, n)
        exchange(send.at[source], recv.at[source], send_sem, recv_sem, d).wait_recv()
    for j in range(n):
        for q in range(block * tiles):
            pixels[j * local : (j + 1) * local, q * LANES : (q + 1) * LANES] = recv[
                j, q * local : (q + 1) * local, :
            ]
    data = pixels[...]

    partial_scatter = dot(data, data, ((1,), (1,)))
    share = epochs // pack
    if pack > 1:
        work[:, 0:epochs] = partial_scatter
        wide = jnp.where(iota((epochs, work.shape[1]), 1) < epochs, work[...], 0.0)[:, 0:LANES]
        packed = wide[0:share, :]
        for j in range(1, pack):
            packed = packed + pltpu.roll(wide[j * share : (j + 1) * share, :], j * epochs, axis=1)
        part[...] = packed
    else:
        part[...] = partial_scatter
    for d in range(1, n):
        exchange(part, parts.at[me], part_send_sem, part_recv_sem, d).start()
    parts[me] = part[...]
    for d in range(1, n):
        source = lax.rem(me - d + n, n)
        exchange(part, parts.at[source], part_send_sem, part_recv_sem, d).wait_recv()
    total = parts[0]
    for j in range(1, n):
        total = total + parts[j]
    if pack > 1:
        pieces = [total] + [
            pltpu.roll(total, LANES - j * epochs, axis=1) for j in range(1, pack)
        ]
        scatter = jnp.concatenate(pieces, axis=0)[:, 0:epochs]
    else:
        scatter = total

    diagonal = iota((epochs, epochs), 0) == iota((epochs, epochs), 1)
    covariance = scatter * (1.0 / npixels) + jnp.where(diagonal, cov_ridge, 0.0)
    work[:, 0:epochs] = covariance + fit_ridge * outer
    work[:, epochs + columns : 2 * epochs + columns] = covariance
    system = work[...]
    index = iota(system.shape, 0)
    for k in range(epochs):
        pivot_row = system[k : k + 1, :]
        factor = system[:, k : k + 1]
        scaled = pivot_row * (1.0 / system[k : k + 1, k : k + 1])
        system = jnp.where(index == k, scaled, system - factor * scaled)

    fitted = dot(system, data, ((0,), (0,)))
    coefficients_ref[...] = fitted[epochs : epochs + columns, :]
    product = dot(scatter, system, ((1,), (0,))) * system
    work[0:1, :] = jnp.sum(product, axis=0, keepdims=True) * (1.0 / npixels)
    epoch_ref[...] = work[0:1, epochs + columns : 2 * epochs + columns]

    for d in range(1, n):
        exchange(send.at[lax.rem(me + d, n)], recv.at[me], send_sem, recv_sem, d).wait_send()
        exchange(part, parts.at[me], part_send_sem, part_recv_sem, d).wait_send()


def ceil_to(value, unit):
    return -(-value // unit) * unit


def solution(mesh):
    n = mesh.shape["ep"]

    def shards(images, reference_image, kernels, kernel_index, tile_mask, systematics, onsets):
        local, rows, width = images.shape
        side = kernels.shape[1]
        tiles = width // LANES
        block = rows // n
        epochs = local * n
        columns = systematics.shape[1] + onsets.shape[0]
        pack = max(LANES // epochs, 1)
        share = epochs // pack
        part_lanes = max(LANES, epochs)
        vmem = pl.BlockSpec(memory_space=pltpu.VMEM)
        smem = pl.BlockSpec(memory_space=pltpu.SMEM)
        dma = pltpu.SemaphoreType.DMA((n,))
        f32 = jnp.float32
        coefficients, epoch_scatter = pl.pallas_call(
            functools.partial(kernel, n),
            out_shape=(
                jax.ShapeDtypeStruct((columns, block * width), f32),
                jax.ShapeDtypeStruct((1, epochs), f32),
            ),
            in_specs=[vmem, vmem, vmem, smem, vmem, vmem, smem],
            out_specs=(vmem, vmem),
            scratch_shapes=[
                pltpu.VMEM((LANES, LANES), f32),
                pltpu.VMEM((LANES, LANES), f32),
                pltpu.VMEM((rows, ceil_to(side * rows, LANES)), f32),
                pltpu.VMEM((ceil_to(side * rows, LANES), width), f32),
                pltpu.VMEM((n, block * tiles * local, LANES), f32),
                pltpu.VMEM((n, block * tiles * local, LANES), f32),
                pltpu.VMEM((epochs, block * width), f32),
                pltpu.VMEM((share, part_lanes), f32),
                pltpu.VMEM((n, share, part_lanes), f32),
                pltpu.VMEM((epochs, ceil_to(2 * epochs + columns, LANES)), f32),
                dma,
                dma,
                dma,
                dma,
            ],
            compiler_params=pltpu.CompilerParams(collective_id=0, has_side_effects=True),
        )(
            images,
            reference_image,
            jnp.transpose(kernels, (1, 0, 2)),
            kernel_index,
            jnp.transpose(tile_mask, (0, 2, 1)),
            systematics,
            onsets,
        )
        return coefficients.reshape(columns, block, width), epoch_scatter.reshape(epochs)

    in_specs = (
        P(("field", "ep"), None, None),
        P("field", None),
        P(),
        P(("field", "ep")),
        P(("field", "ep"), None, None),
        P("field", None),
        P("field"),
    )
    out_specs = (P(None, ("field", "ep"), None), P("field"))
    return jax.shard_map(shards, mesh=mesh, in_specs=in_specs, out_specs=out_specs, check_vma=False)
```

```python
import functools

import jax
import jax.numpy as jnp
from jax import lax
from jax.experimental import pallas as pl
from jax.experimental.pallas import tpu as pltpu
from jax.sharding import PartitionSpec as P

cov_ridge = 0.5
fit_ridge = 1.0
LANES = 128
VMEM_GRANT = 24 * 2**20
HIGHEST = lax.Precision.HIGHEST


def dot(a, b, contract):
    return lax.dot_general(
        a, b, ((contract[0], contract[1]), ((), ())), precision=HIGHEST, preferred_element_type=jnp.float32
    )


def iota(shape, axis):
    return lax.broadcasted_iota(jnp.int32, shape, axis)


def exchange_kernel(
    n,
    images_hbm,
    reference_hbm,
    kernels_hbm,
    index_hbm,
    mask_hbm,
    systematics_hbm,
    onsets_hbm,
    pixels,
    total_ref,
    work,
    images_ref,
    reference_ref,
    kernels_ref,
    index_ref,
    mask_ref,
    systematics_ref,
    onsets_ref,
    table,
    table_t,
    taps,
    shifted,
    send,
    recv,
    part,
    parts,
    load_sem,
    send_sem,
    recv_sem,
    part_send_sem,
    part_recv_sem,
):
    local, rows, width = images_ref.shape
    side = kernels_ref.shape[0]
    half = (side - 1) // 2
    tiles = width // LANES
    block = rows // n
    epochs = local * n
    nsys = systematics_ref.shape[1]
    ntr = onsets_ref.shape[0]
    columns = nsys + ntr
    pack = max(LANES // epochs, 1)
    me = lax.axis_index("ep")

    barrier = pltpu.get_barrier_semaphore()
    for d in range(1, n):
        pl.semaphore_signal(
            barrier,
            inc=1,
            device_id={"ep": lax.rem(me + d, n)},
            device_id_type=pl.DeviceIdType.MESH,
        )

    loads = [
        pltpu.make_async_copy(source, target, load_sem.at[i])
        for i, (source, target) in enumerate(
            (
                (index_hbm, index_ref),
                (kernels_hbm, kernels_ref),
                (images_hbm, images_ref),
                (mask_hbm, mask_ref),
                (reference_hbm, reference_ref),
                (systematics_hbm, systematics_ref),
                (onsets_hbm, onsets_ref),
            )
        )
    ]
    for load in loads:
        load.start()
    for load in loads:
        load.wait()

    depth = side * rows
    padded_depth = taps.shape[1]
    lane = iota((rows, LANES), 1)
    column = iota((rows, width), 1)
    for e in range(local):
        table[...] = jnp.zeros_like(table)
        for a in range(side):
            table[a : a + 1, 0:side] = kernels_ref[a, pl.ds(index_ref[e], 1), :]
        table[side + 1 : side + 1 + tiles, 0:rows] = mask_ref[e].astype(jnp.float32)
        table_t[...] = table[...].T
        kept = jnp.where(iota((side, LANES), 1) < side, table_t[0:side, :], 0.0)
        kept = pltpu.roll(kept, LANES - half, axis=1)
        groups = [jnp.zeros((rows, LANES), jnp.float32) for _ in range(padded_depth // LANES)]
        for b in range(side):
            start = b * rows
            at = start % LANES
            row = jnp.broadcast_to(kept[b : b + 1, :], (rows, LANES))
            turned = pltpu.roll(row, at, axis=1, stride=1, stride_axis=0)
            inside = (lane >= at) & (lane < at + rows)
            groups[start // LANES] = jnp.where(inside, turned, groups[start // LANES])
        for g, value in enumerate(groups):
            taps[:, g * LANES : (g + 1) * LANES] = value
        image = images_ref[e]
        for b in range(side):
            move = b - half
            moved = pltpu.roll(image, (-move) % width, axis=1) if move else image
            inside = (column + move >= 0) & (column + move < width)
            shifted[b * rows : (b + 1) * rows, :] = jnp.where(inside, moved, 0.0)
        if padded_depth > depth:
            shifted[depth:, :] = jnp.zeros((padded_depth - depth, width), jnp.float32)
        difference = reference_ref[...] - dot(taps[...], shifted[...], ((1,), (0,)))
        for t in range(tiles):
            good = table_t[0:rows, side + 1 + t : side + 2 + t]
            piece = difference[:, t * LANES : (t + 1) * LANES] * good
            for r in range(rows):
                slot = (r % block) * tiles * local + t * local + e
                send[r // block, slot : slot + 1, :] = piece[r : r + 1, :]

    pl.semaphore_wait(barrier, n - 1)

    def exchange(source, target, send_sems, recv_sems, d):
        return pltpu.make_async_remote_copy(
            src_ref=source,
            dst_ref=target,
            send_sem=send_sems.at[d],
            recv_sem=recv_sems.at[d],
            device_id={"ep": lax.rem(me + d, n)},
            device_id_type=pl.DeviceIdType.MESH,
        )

    for d in range(1, n):
        exchange(send.at[lax.rem(me + d, n)], recv.at[me], send_sem, recv_sem, d).start()
    recv[me] = send[me]

    work[...] = jnp.zeros_like(work)
    epoch = iota((epochs, LANES), 0).astype(jnp.float32)
    template = iota((epochs, LANES), 1)
    onset = jnp.zeros((epochs, LANES), jnp.float32)
    for k in range(ntr):
        onset = jnp.where(template == k, onsets_ref[k].astype(jnp.float32), onset)
    delays = epoch - onset
    timescale = (template.astype(jnp.float32) + 1.0) * epochs / (2.0 * ntr)
    transient = jnp.where(delays >= 0.0, jnp.exp(-jnp.maximum(delays, 0.0) / timescale), 0.0)
    work[:, epochs : epochs + nsys] = systematics_ref[...]
    work[:, epochs + nsys : epochs + columns] = transient[:, 0:ntr]
    design = work[...]
    outer = dot(design, design, ((1,), (1,)))
    diagonal = iota((epochs, epochs), 0) == iota((epochs, epochs), 1)
    ridge = jnp.where(diagonal, cov_ridge, 0.0)

    for d in range(1, n):
        source = lax.rem(me - d + n, n)
        exchange(send.at[source], recv.at[source], send_sem, recv_sem, d).wait_recv()
    for j in range(n):
        for q in range(block * tiles):
            pixels[j * local : (j + 1) * local, q * LANES : (q + 1) * LANES] = recv[
                j, q * local : (q + 1) * local, :
            ]
    data = pixels[...]

    partial_scatter = dot(data, data, ((1,), (1,)))
    share = epochs // pack
    if pack > 1:
        table[0:epochs, :] = jnp.zeros((epochs, LANES), jnp.float32)
        table[0:epochs, 0:epochs] = partial_scatter
        wide = table[0:epochs, :]
        packed = wide[0:share, :]
        for j in range(1, pack):
            packed = packed + pltpu.roll(wide[j * share : (j + 1) * share, :], j * epochs, axis=1)
        part[...] = packed
    else:
        part[...] = partial_scatter
    for d in range(1, n):
        exchange(part, parts.at[me], part_send_sem, part_recv_sem, d).start()
    parts[me] = part[...]
    for d in range(1, n):
        source = lax.rem(me - d + n, n)
        exchange(part, parts.at[source], part_send_sem, part_recv_sem, d).wait_recv()
    total = parts[0]
    for j in range(1, n):
        total = total + parts[j]
    total_ref[...] = total
    work[:, 0:epochs] = fit_ridge * outer + ridge
    work[:, epochs + columns : 2 * epochs + columns] = ridge

    for d in range(1, n):
        exchange(send.at[lax.rem(me + d, n)], recv.at[me], send_sem, recv_sem, d).wait_send()
        exchange(part, parts.at[me], part_send_sem, part_recv_sem, d).wait_send()


def fit_kernel(npixels, pixels_ref, total_ref, base_ref, coefficients_ref, epoch_ref, work):
    columns, block, width = coefficients_ref.shape
    epochs = pixels_ref.shape[0]
    pack = epochs // total_ref.shape[0]
    total = total_ref[...]
    if pack > 1:
        pieces = [total] + [
            pltpu.roll(total, LANES - j * epochs, axis=1) for j in range(1, pack)
        ]
        scatter = jnp.concatenate(pieces, axis=0)[:, 0:epochs]
    else:
        scatter = total

    covariance = scatter * (1.0 / npixels)
    work[...] = jnp.zeros_like(work)
    work[:, 0:epochs] = covariance
    work[:, epochs + columns : 2 * epochs + columns] = covariance
    system = work[...] + base_ref[...]
    index = iota(system.shape, 0)
    for k in range(epochs):
        pivot_row = system[k : k + 1, :]
        factor = system[:, k : k + 1]
        scaled = pivot_row * (1.0 / system[k : k + 1, k : k + 1])
        system = jnp.where(index == k, scaled, system - factor * scaled)

    fitted = dot(system, pixels_ref[...], ((0,), (0,)))[epochs : epochs + columns, :]
    for q in range(block):
        coefficients_ref[:, q, :] = fitted[:, q * width : (q + 1) * width]
    product = dot(scatter, system, ((1,), (0,))) * system
    work[0:1, :] = jnp.sum(product, axis=0, keepdims=True) * (1.0 / npixels)
    epoch_ref[...] = work[0, epochs + columns : 2 * epochs + columns]


def ceil_to(value, unit):
    return -(-value // unit) * unit


def solution(mesh):
    n = mesh.shape["ep"]

    def shards(images, reference_image, kernels, kernel_index, tile_mask, systematics, onsets):
        local, rows, width = images.shape
        side = kernels.shape[1]
        tiles = width // LANES
        block = rows // n
        epochs = local * n
        columns = systematics.shape[1] + onsets.shape[0]
        pack = max(LANES // epochs, 1)
        share = epochs // pack
        part_lanes = max(LANES, epochs)
        vmem = pl.BlockSpec(memory_space=pltpu.VMEM)
        dma = pltpu.SemaphoreType.DMA((n,))
        f32 = jnp.float32
        flat_kernels = jnp.transpose(kernels, (1, 0, 2))
        flat_mask = jnp.transpose(tile_mask, (0, 2, 1))
        system_lanes = ceil_to(2 * epochs + columns, LANES)
        pixels, total, base = pl.pallas_call(
            functools.partial(exchange_kernel, n),
            out_shape=(
                jax.ShapeDtypeStruct((epochs, block * width), f32),
                jax.ShapeDtypeStruct((share, part_lanes), f32),
                jax.ShapeDtypeStruct((epochs, system_lanes), f32),
            ),
            in_specs=[pl.BlockSpec(memory_space=pltpu.HBM)] * 7,
            out_specs=(vmem, vmem, vmem),
            scratch_shapes=[
                pltpu.VMEM(images.shape, f32),
                pltpu.VMEM(reference_image.shape, f32),
                pltpu.VMEM(flat_kernels.shape, f32),
                pltpu.SMEM(kernel_index.shape, jnp.int32),
                pltpu.VMEM(flat_mask.shape, jnp.int32),
                pltpu.VMEM(systematics.shape, f32),
                pltpu.SMEM(onsets.shape, jnp.int32),
                pltpu.VMEM((LANES, LANES), f32),
                pltpu.VMEM((LANES, LANES), f32),
                pltpu.VMEM((rows, ceil_to(side * rows, LANES)), f32),
                pltpu.VMEM((ceil_to(side * rows, LANES), width), f32),
                pltpu.VMEM((n, block * tiles * local, LANES), f32),
                pltpu.VMEM((n, block * tiles * local, LANES), f32),
                pltpu.VMEM((share, part_lanes), f32),
                pltpu.VMEM((n, share, part_lanes), f32),
                pltpu.SemaphoreType.DMA((7,)),
                dma,
                dma,
                dma,
                dma,
            ],
            compiler_params=pltpu.CompilerParams(
                collective_id=0, has_side_effects=True, vmem_limit_bytes=VMEM_GRANT
            ),
        )(
            *(
                pltpu.with_memory_space_constraint(value, pltpu.HBM)
                for value in (
                    images,
                    reference_image,
                    flat_kernels,
                    kernel_index,
                    flat_mask,
                    systematics,
                    onsets,
                )
            )
        )
        return pl.pallas_call(
            functools.partial(fit_kernel, float(rows * width)),
            out_shape=(
                jax.ShapeDtypeStruct((columns, block, width), f32),
                jax.ShapeDtypeStruct((epochs,), f32),
            ),
            in_specs=[vmem, vmem, vmem],
            out_specs=(vmem, vmem),
            scratch_shapes=[pltpu.VMEM((epochs, system_lanes), f32)],
            compiler_params=pltpu.CompilerParams(vmem_limit_bytes=VMEM_GRANT),
        )(pixels, total, base)

    in_specs = (
        P(("field", "ep"), None, None),
        P("field", None),
        P(),
        P(("field", "ep")),
        P(("field", "ep"), None, None),
        P("field", None),
        P("field"),
    )
    out_specs = (P(None, ("field", "ep"), None), P("field"))
    return jax.shard_map(shards, mesh=mesh, in_specs=in_specs, out_specs=out_specs, check_vma=False)
```

```python
import functools

import jax
import jax.numpy as jnp
from jax import lax
from jax.experimental import pallas as pl
from jax.experimental.pallas import tpu as pltpu
from jax.sharding import PartitionSpec as P

cov_ridge = 0.5
fit_ridge = 1.0
LANES = 128
VMEM_GRANT = 24 * 2**20
HIGHEST = lax.Precision.HIGHEST


def dot(a, b, contract):
    return lax.dot_general(
        a, b, ((contract[0], contract[1]), ((), ())), precision=HIGHEST, preferred_element_type=jnp.float32
    )


def iota(shape, axis):
    return lax.broadcasted_iota(jnp.int32, shape, axis)


def exchange_kernel(
    n,
    images_hbm,
    reference_hbm,
    kernels_hbm,
    index_hbm,
    mask_hbm,
    systematics_hbm,
    onsets_hbm,
    pixels,
    total_ref,
    work,
    images_ref,
    reference_ref,
    kernels_ref,
    index_ref,
    mask_ref,
    systematics_ref,
    onsets_ref,
    table,
    table_t,
    taps,
    shifted,
    send,
    recv,
    part,
    parts,
    load_sem,
    send_sem,
    recv_sem,
    part_send_sem,
    part_recv_sem,
):
    local, rows, width = images_ref.shape
    side = kernels_ref.shape[0]
    half = (side - 1) // 2
    tiles = width // LANES
    block = rows // n
    epochs = local * n
    nsys = systematics_ref.shape[1]
    ntr = onsets_ref.shape[0]
    columns = nsys + ntr
    pack = max(LANES // epochs, 1)
    me = lax.axis_index("ep")

    barrier = pltpu.get_barrier_semaphore()
    for d in range(1, n):
        pl.semaphore_signal(
            barrier,
            inc=1,
            device_id={"ep": lax.rem(me + d, n)},
            device_id_type=pl.DeviceIdType.MESH,
        )

    loads = [
        pltpu.make_async_copy(source, target, load_sem.at[i])
        for i, (source, target) in enumerate(
            (
                (index_hbm, index_ref),
                (kernels_hbm, kernels_ref),
                (images_hbm, images_ref),
                (mask_hbm, mask_ref),
                (reference_hbm, reference_ref),
                (systematics_hbm, systematics_ref),
                (onsets_hbm, onsets_ref),
            )
        )
    ]
    for load in loads:
        load.start()
    for load in loads:
        load.wait()

    depth = side * rows
    padded_depth = taps.shape[1]
    lane = iota((rows, LANES), 1)
    column = iota((rows, width), 1)
    for e in range(local):
        table[...] = jnp.zeros_like(table)
        for a in range(side):
            table[a : a + 1, 0:side] = kernels_ref[a, pl.ds(index_ref[e], 1), :]
        table[side + 1 : side + 1 + tiles, 0:rows] = mask_ref[e].astype(jnp.float32)
        table_t[...] = table[...].T
        kept = jnp.where(iota((side, LANES), 1) < side, table_t[0:side, :], 0.0)
        kept = pltpu.roll(kept, LANES - half, axis=1)
        groups = [jnp.zeros((rows, LANES), jnp.float32) for _ in range(padded_depth // LANES)]
        for b in range(side):
            start = b * rows
            at = start % LANES
            row = jnp.broadcast_to(kept[b : b + 1, :], (rows, LANES))
            turned = pltpu.roll(row, at, axis=1, stride=1, stride_axis=0)
            inside = (lane >= at) & (lane < at + rows)
            groups[start // LANES] = jnp.where(inside, turned, groups[start // LANES])
        for g, value in enumerate(groups):
            taps[:, g * LANES : (g + 1) * LANES] = value
        image = images_ref[e]
        for b in range(side):
            move = b - half
            moved = pltpu.roll(image, (-move) % width, axis=1) if move else image
            inside = (column + move >= 0) & (column + move < width)
            shifted[b * rows : (b + 1) * rows, :] = jnp.where(inside, moved, 0.0)
        if padded_depth > depth:
            shifted[depth:, :] = jnp.zeros((padded_depth - depth, width), jnp.float32)
        difference = reference_ref[...] - dot(taps[...], shifted[...], ((1,), (0,)))
        for t in range(tiles):
            good = table_t[0:rows, side + 1 + t : side + 2 + t]
            piece = difference[:, t * LANES : (t + 1) * LANES] * good
            for r in range(rows):
                slot = (r % block) * tiles * local + t * local + e
                send[r // block, slot : slot + 1, :] = piece[r : r + 1, :]

    pl.semaphore_wait(barrier, n - 1)

    def exchange(source, target, send_sems, recv_sems, d):
        return pltpu.make_async_remote_copy(
            src_ref=source,
            dst_ref=target,
            send_sem=send_sems.at[d],
            recv_sem=recv_sems.at[d],
            device_id={"ep": lax.rem(me + d, n)},
            device_id_type=pl.DeviceIdType.MESH,
        )

    for d in range(1, n):
        exchange(send.at[lax.rem(me + d, n)], recv.at[me], send_sem, recv_sem, d).start()
    recv[me] = send[me]

    work[...] = jnp.zeros_like(work)
    epoch = iota((epochs, LANES), 0).astype(jnp.float32)
    template = iota((epochs, LANES), 1)
    onset = jnp.zeros((epochs, LANES), jnp.float32)
    for k in range(ntr):
        onset = jnp.where(template == k, onsets_ref[k].astype(jnp.float32), onset)
    delays = epoch - onset
    timescale = (template.astype(jnp.float32) + 1.0) * epochs / (2.0 * ntr)
    transient = jnp.where(delays >= 0.0, jnp.exp(-jnp.maximum(delays, 0.0) / timescale), 0.0)
    work[:, epochs : epochs + nsys] = systematics_ref[...]
    work[:, epochs + nsys : epochs + columns] = transient[:, 0:ntr]
    design = work[...]
    outer = dot(design, design, ((1,), (1,)))
    diagonal = iota((epochs, epochs), 0) == iota((epochs, epochs), 1)
    ridge = jnp.where(diagonal, cov_ridge, 0.0)

    for d in range(1, n):
        source = lax.rem(me - d + n, n)
        exchange(send.at[source], recv.at[source], send_sem, recv_sem, d).wait_recv()
    for j in range(n):
        for q in range(block * tiles):
            pixels[j * local : (j + 1) * local, q * LANES : (q + 1) * LANES] = recv[
                j, q * local : (q + 1) * local, :
            ]
    data = pixels[...]

    partial_scatter = dot(data, data, ((1,), (1,)))
    share = epochs // pack
    if pack > 1:
        table[0:epochs, :] = jnp.zeros((epochs, LANES), jnp.float32)
        table[0:epochs, 0:epochs] = partial_scatter
        wide = table[0:epochs, :]
        packed = wide[0:share, :]
        for j in range(1, pack):
            packed = packed + pltpu.roll(wide[j * share : (j + 1) * share, :], j * epochs, axis=1)
        part[...] = packed
    else:
        part[...] = partial_scatter
    for d in range(1, n):
        exchange(part, parts.at[me], part_send_sem, part_recv_sem, d).start()
    parts[me] = part[...]
    for d in range(1, n):
        source = lax.rem(me - d + n, n)
        exchange(part, parts.at[source], part_send_sem, part_recv_sem, d).wait_recv()
    total = parts[0]
    for j in range(1, n):
        total = total + parts[j]
    total_ref[...] = total
    work[:, 0:epochs] = fit_ridge * outer + ridge
    work[:, epochs + columns : 2 * epochs + columns] = ridge

    for d in range(1, n):
        exchange(send.at[lax.rem(me + d, n)], recv.at[me], send_sem, recv_sem, d).wait_send()
        exchange(part, parts.at[me], part_send_sem, part_recv_sem, d).wait_send()


def fit_kernel(npixels, pixels_ref, total_ref, base_ref, coefficients_ref, epoch_ref, work):
    columns, block, width = coefficients_ref.shape
    epochs = pixels_ref.shape[0]
    pack = epochs // total_ref.shape[0]
    total = total_ref[...]
    if pack > 1:
        pieces = [total] + [
            pltpu.roll(total, LANES - j * epochs, axis=1) for j in range(1, pack)
        ]
        scatter = jnp.concatenate(pieces, axis=0)[:, 0:epochs]
    else:
        scatter = total

    covariance = scatter * (1.0 / npixels)
    work[...] = jnp.zeros_like(work)
    work[:, 0:epochs] = covariance
    work[:, epochs + columns : 2 * epochs + columns] = covariance
    system = work[...] + base_ref[...]
    lanes = system.shape[1]
    group = (8, lanes)
    strips = [system[i : i + 8, :] for i in range(0, epochs, 8)]
    index = iota(group, 0)

    def spread(value, row):
        return jnp.broadcast_to(value[row : row + 1, :], group)

    for home in range(epochs // 8):
        spans = [
            [jnp.broadcast_to(strip[:, k : k + 1], group) for strip in strips]
            for k in range(home * 8, home * 8 + 8)
        ]
        for row in range(8):
            factors = spans[row]
            inverse = 1.0 / spread(factors[home], row)

            def step(values):
                scaled = spread(values[home], row) * inverse
                values = [v - f * scaled for v, f in zip(values, factors)]
                values[home] = jnp.where(index == row, scaled, values[home])
                return values

            spans = [step(span) if j > row else span for j, span in enumerate(spans)]
            strips = step(strips)
    system = jnp.concatenate(strips, axis=0)

    fitted = dot(system, pixels_ref[...], ((0,), (0,)))[epochs : epochs + columns, :]
    for q in range(block):
        coefficients_ref[:, q, :] = fitted[:, q * width : (q + 1) * width]
    product = dot(scatter, system, ((1,), (0,))) * system
    work[0:1, :] = jnp.sum(product, axis=0, keepdims=True) * (1.0 / npixels)
    epoch_ref[...] = work[0, epochs + columns : 2 * epochs + columns]


def ceil_to(value, unit):
    return -(-value // unit) * unit


def solution(mesh):
    n = mesh.shape["ep"]

    def shards(images, reference_image, kernels, kernel_index, tile_mask, systematics, onsets):
        local, rows, width = images.shape
        side = kernels.shape[1]
        tiles = width // LANES
        block = rows // n
        epochs = local * n
        columns = systematics.shape[1] + onsets.shape[0]
        pack = max(LANES // epochs, 1)
        share = epochs // pack
        part_lanes = max(LANES, epochs)
        vmem = pl.BlockSpec(memory_space=pltpu.VMEM)
        dma = pltpu.SemaphoreType.DMA((n,))
        f32 = jnp.float32
        flat_kernels = jnp.transpose(kernels, (1, 0, 2))
        flat_mask = jnp.transpose(tile_mask, (0, 2, 1))
        system_lanes = ceil_to(2 * epochs + columns, LANES)
        pixels, total, base = pl.pallas_call(
            functools.partial(exchange_kernel, n),
            out_shape=(
                jax.ShapeDtypeStruct((epochs, block * width), f32),
                jax.ShapeDtypeStruct((share, part_lanes), f32),
                jax.ShapeDtypeStruct((epochs, system_lanes), f32),
            ),
            in_specs=[pl.BlockSpec(memory_space=pltpu.HBM)] * 7,
            out_specs=(vmem, vmem, vmem),
            scratch_shapes=[
                pltpu.VMEM(images.shape, f32),
                pltpu.VMEM(reference_image.shape, f32),
                pltpu.VMEM(flat_kernels.shape, f32),
                pltpu.SMEM(kernel_index.shape, jnp.int32),
                pltpu.VMEM(flat_mask.shape, jnp.int32),
                pltpu.VMEM(systematics.shape, f32),
                pltpu.SMEM(onsets.shape, jnp.int32),
                pltpu.VMEM((LANES, LANES), f32),
                pltpu.VMEM((LANES, LANES), f32),
                pltpu.VMEM((rows, ceil_to(side * rows, LANES)), f32),
                pltpu.VMEM((ceil_to(side * rows, LANES), width), f32),
                pltpu.VMEM((n, block * tiles * local, LANES), f32),
                pltpu.VMEM((n, block * tiles * local, LANES), f32),
                pltpu.VMEM((share, part_lanes), f32),
                pltpu.VMEM((n, share, part_lanes), f32),
                pltpu.SemaphoreType.DMA((7,)),
                dma,
                dma,
                dma,
                dma,
            ],
            compiler_params=pltpu.CompilerParams(
                collective_id=0, has_side_effects=True, vmem_limit_bytes=VMEM_GRANT
            ),
        )(
            *(
                pltpu.with_memory_space_constraint(value, pltpu.HBM)
                for value in (
                    images,
                    reference_image,
                    flat_kernels,
                    kernel_index,
                    flat_mask,
                    systematics,
                    onsets,
                )
            )
        )
        return pl.pallas_call(
            functools.partial(fit_kernel, float(rows * width)),
            out_shape=(
                jax.ShapeDtypeStruct((columns, block, width), f32),
                jax.ShapeDtypeStruct((epochs,), f32),
            ),
            in_specs=[vmem, vmem, vmem],
            out_specs=(vmem, vmem),
            scratch_shapes=[pltpu.VMEM((epochs, system_lanes), f32)],
            compiler_params=pltpu.CompilerParams(vmem_limit_bytes=VMEM_GRANT),
        )(pixels, total, base)

    in_specs = (
        P(("field", "ep"), None, None),
        P("field", None),
        P(),
        P(("field", "ep")),
        P(("field", "ep"), None, None),
        P("field", None),
        P("field"),
    )
    out_specs = (P(None, ("field", "ep"), None), P("field"))
    return jax.shard_map(shards, mesh=mesh, in_specs=in_specs, out_specs=out_specs, check_vma=False)
```

```python
import functools

import jax
import jax.numpy as jnp
from jax import lax
from jax.experimental import pallas as pl
from jax.experimental.pallas import tpu as pltpu
from jax.sharding import PartitionSpec as P

cov_ridge = 0.5
fit_ridge = 1.0
LANES = 128
VMEM_GRANT = 24 * 2**20
HIGHEST = lax.Precision.HIGHEST


def dot(a, b, contract):
    return lax.dot_general(
        a, b, ((contract[0], contract[1]), ((), ())), precision=HIGHEST, preferred_element_type=jnp.float32
    )


def iota(shape, axis):
    return lax.broadcasted_iota(jnp.int32, shape, axis)


def exchange_kernel(
    n,
    images_hbm,
    reference_hbm,
    kernels_hbm,
    index_hbm,
    mask_hbm,
    systematics_hbm,
    onsets_hbm,
    pixels,
    total_ref,
    work,
    images_ref,
    reference_ref,
    kernels_ref,
    index_ref,
    mask_ref,
    systematics_ref,
    onsets_ref,
    table,
    table_t,
    taps,
    shifted,
    send,
    recv,
    part,
    parts,
    load_sem,
    send_sem,
    recv_sem,
    part_send_sem,
    part_recv_sem,
):
    local, rows, width = images_ref.shape
    side = kernels_ref.shape[0]
    half = (side - 1) // 2
    tiles = width // LANES
    block = rows // n
    epochs = local * n
    nsys = systematics_ref.shape[1]
    ntr = onsets_ref.shape[0]
    columns = nsys + ntr
    pack = max(LANES // epochs, 1)
    me = lax.axis_index("ep")

    barrier = pltpu.get_barrier_semaphore()
    for d in range(1, n):
        pl.semaphore_signal(
            barrier,
            inc=1,
            device_id={"ep": lax.rem(me + d, n)},
            device_id_type=pl.DeviceIdType.MESH,
        )

    loads = [
        pltpu.make_async_copy(source, target, load_sem.at[i])
        for i, (source, target) in enumerate(
            (
                (index_hbm, index_ref),
                (kernels_hbm, kernels_ref),
                (images_hbm, images_ref),
                (mask_hbm, mask_ref),
                (reference_hbm, reference_ref),
                (systematics_hbm, systematics_ref),
                (onsets_hbm, onsets_ref),
            )
        )
    ]
    for load in loads:
        load.start()
    for load in loads:
        load.wait()

    depth = side * rows
    padded_depth = taps.shape[1]
    lane = iota((rows, LANES), 1)
    column = iota((rows, width), 1)
    for e in range(local):
        table[...] = jnp.zeros_like(table)
        for a in range(side):
            table[a : a + 1, 0:side] = kernels_ref[a, pl.ds(index_ref[e], 1), :]
        table[side + 1 : side + 1 + tiles, 0:rows] = mask_ref[e].astype(jnp.float32)
        table_t[...] = table[...].T
        kept = jnp.where(iota((side, LANES), 1) < side, table_t[0:side, :], 0.0)
        kept = pltpu.roll(kept, LANES - half, axis=1)
        groups = [jnp.zeros((rows, LANES), jnp.float32) for _ in range(padded_depth // LANES)]
        for b in range(side):
            start = b * rows
            at = start % LANES
            row = jnp.broadcast_to(kept[b : b + 1, :], (rows, LANES))
            turned = pltpu.roll(row, at, axis=1, stride=1, stride_axis=0)
            inside = (lane >= at) & (lane < at + rows)
            groups[start // LANES] = jnp.where(inside, turned, groups[start // LANES])
        for g, value in enumerate(groups):
            taps[:, g * LANES : (g + 1) * LANES] = value
        image = images_ref[e]
        for b in range(side):
            move = b - half
            moved = pltpu.roll(image, (-move) % width, axis=1) if move else image
            inside = (column + move >= 0) & (column + move < width)
            shifted[b * rows : (b + 1) * rows, :] = jnp.where(inside, moved, 0.0)
        if padded_depth > depth:
            shifted[depth:, :] = jnp.zeros((padded_depth - depth, width), jnp.float32)
        difference = reference_ref[...] - dot(taps[...], shifted[...], ((1,), (0,)))
        for t in range(tiles):
            good = table_t[0:rows, side + 1 + t : side + 2 + t]
            piece = difference[:, t * LANES : (t + 1) * LANES] * good
            for r in range(rows):
                slot = (r % block) * tiles * local + t * local + e
                send[r // block, slot : slot + 1, :] = piece[r : r + 1, :]

    pl.semaphore_wait(barrier, n - 1)

    def exchange(source, target, send_sems, recv_sems, d):
        return pltpu.make_async_remote_copy(
            src_ref=source,
            dst_ref=target,
            send_sem=send_sems.at[d],
            recv_sem=recv_sems.at[d],
            device_id={"ep": lax.rem(me + d, n)},
            device_id_type=pl.DeviceIdType.MESH,
        )

    for d in (*range(2, n, 2), *range(1, n, 2)):
        exchange(send.at[lax.rem(me + d, n)], recv.at[me], send_sem, recv_sem, d).start()
    recv[me] = send[me]

    work[...] = jnp.zeros_like(work)
    epoch = iota((epochs, LANES), 0).astype(jnp.float32)
    template = iota((epochs, LANES), 1)
    onset = jnp.zeros((epochs, LANES), jnp.float32)
    for k in range(ntr):
        onset = jnp.where(template == k, onsets_ref[k].astype(jnp.float32), onset)
    delays = epoch - onset
    timescale = (template.astype(jnp.float32) + 1.0) * epochs / (2.0 * ntr)
    transient = jnp.where(delays >= 0.0, jnp.exp(-jnp.maximum(delays, 0.0) / timescale), 0.0)
    work[:, epochs : epochs + nsys] = systematics_ref[...]
    work[:, epochs + nsys : epochs + columns] = transient[:, 0:ntr]
    design = work[...]
    outer = dot(design, design, ((1,), (1,)))
    diagonal = iota((epochs, epochs), 0) == iota((epochs, epochs), 1)
    ridge = jnp.where(diagonal, cov_ridge, 0.0)

    for d in range(1, n):
        source = lax.rem(me - d + n, n)
        exchange(send.at[source], recv.at[source], send_sem, recv_sem, d).wait_recv()
    for j in range(n):
        for q in range(block * tiles):
            pixels[j * local : (j + 1) * local, q * LANES : (q + 1) * LANES] = recv[
                j, q * local : (q + 1) * local, :
            ]
    data = pixels[...]

    partial_scatter = dot(data, data, ((1,), (1,)))
    share = epochs // pack
    if pack > 1:
        table[0:epochs, :] = jnp.zeros((epochs, LANES), jnp.float32)
        table[0:epochs, 0:epochs] = partial_scatter
        wide = table[0:epochs, :]
        packed = wide[0:share, :]
        for j in range(1, pack):
            packed = packed + pltpu.roll(wide[j * share : (j + 1) * share, :], j * epochs, axis=1)
        part[...] = packed
    else:
        part[...] = partial_scatter
    for d in (*range(2, n, 2), *range(1, n, 2)):
        exchange(part, parts.at[me], part_send_sem, part_recv_sem, d).start()
    parts[me] = part[...]
    for d in range(1, n):
        source = lax.rem(me - d + n, n)
        exchange(part, parts.at[source], part_send_sem, part_recv_sem, d).wait_recv()
    total = parts[0]
    for j in range(1, n):
        total = total + parts[j]
    total_ref[...] = total
    work[:, 0:epochs] = fit_ridge * outer + ridge
    work[:, epochs + columns : 2 * epochs + columns] = ridge

    for d in range(1, n):
        exchange(send.at[lax.rem(me + d, n)], recv.at[me], send_sem, recv_sem, d).wait_send()
        exchange(part, parts.at[me], part_send_sem, part_recv_sem, d).wait_send()


def fit_kernel(npixels, pixels_ref, total_ref, base_ref, coefficients_ref, epoch_ref, work):
    columns, block, width = coefficients_ref.shape
    epochs = pixels_ref.shape[0]
    pack = epochs // total_ref.shape[0]
    total = total_ref[...]
    if pack > 1:
        pieces = [total] + [
            pltpu.roll(total, LANES - j * epochs, axis=1) for j in range(1, pack)
        ]
        scatter = jnp.concatenate(pieces, axis=0)[:, 0:epochs]
    else:
        scatter = total

    covariance = scatter * (1.0 / npixels)
    work[...] = jnp.zeros_like(work)
    work[:, 0:epochs] = covariance
    work[:, epochs + columns : 2 * epochs + columns] = covariance
    system = work[...] + base_ref[...]
    lanes = system.shape[1]
    group = (8, lanes)
    strips = [system[i : i + 8, :] for i in range(0, epochs, 8)]
    index = iota(group, 0)

    def spread(value, row):
        return jnp.broadcast_to(value[row : row + 1, :], group)

    for home in range(epochs // 8):
        spans = [
            [jnp.broadcast_to(strip[:, k : k + 1], group) for strip in strips]
            for k in range(home * 8, home * 8 + 8)
        ]
        for row in range(0, 8, 2):
            lefts, rights = spans[row], spans[row + 1]
            a, b = spread(lefts[home], row), spread(rights[home], row)
            c, d = spread(lefts[home], row + 1), spread(rights[home], row + 1)
            inverse = 1.0 / (a * d - b * c)

            def step(values):
                first, second = spread(values[home], row), spread(values[home], row + 1)
                upper = (d * first - b * second) * inverse
                lower = (a * second - c * first) * inverse
                values = [
                    v - left * upper - right * lower
                    for v, left, right in zip(values, lefts, rights)
                ]
                values[home] = jnp.where(
                    index == row, upper, jnp.where(index == row + 1, lower, values[home])
                )
                return values

            spans = [step(span) if j > row + 1 else span for j, span in enumerate(spans)]
            strips = step(strips)
    system = jnp.concatenate(strips, axis=0)

    fitted = dot(system, pixels_ref[...], ((0,), (0,)))[epochs : epochs + columns, :]
    for q in range(block):
        coefficients_ref[:, q, :] = fitted[:, q * width : (q + 1) * width]
    product = dot(scatter, system, ((1,), (0,))) * system
    work[0:1, :] = jnp.sum(product, axis=0, keepdims=True) * (1.0 / npixels)
    epoch_ref[...] = work[0, epochs + columns : 2 * epochs + columns]


def ceil_to(value, unit):
    return -(-value // unit) * unit


def solution(mesh):
    n = mesh.shape["ep"]

    def shards(images, reference_image, kernels, kernel_index, tile_mask, systematics, onsets):
        local, rows, width = images.shape
        side = kernels.shape[1]
        tiles = width // LANES
        block = rows // n
        epochs = local * n
        columns = systematics.shape[1] + onsets.shape[0]
        pack = max(LANES // epochs, 1)
        share = epochs // pack
        part_lanes = max(LANES, epochs)
        vmem = pl.BlockSpec(memory_space=pltpu.VMEM)
        dma = pltpu.SemaphoreType.DMA((n,))
        f32 = jnp.float32
        flat_kernels = jnp.transpose(kernels, (1, 0, 2))
        flat_mask = jnp.transpose(tile_mask, (0, 2, 1))
        system_lanes = ceil_to(2 * epochs + columns, LANES)
        pixels, total, base = pl.pallas_call(
            functools.partial(exchange_kernel, n),
            out_shape=(
                jax.ShapeDtypeStruct((epochs, block * width), f32),
                jax.ShapeDtypeStruct((share, part_lanes), f32),
                jax.ShapeDtypeStruct((epochs, system_lanes), f32),
            ),
            in_specs=[pl.BlockSpec(memory_space=pltpu.HBM)] * 7,
            out_specs=(vmem, vmem, vmem),
            scratch_shapes=[
                pltpu.VMEM(images.shape, f32),
                pltpu.VMEM(reference_image.shape, f32),
                pltpu.VMEM(flat_kernels.shape, f32),
                pltpu.SMEM(kernel_index.shape, jnp.int32),
                pltpu.VMEM(flat_mask.shape, jnp.int32),
                pltpu.VMEM(systematics.shape, f32),
                pltpu.SMEM(onsets.shape, jnp.int32),
                pltpu.VMEM((LANES, LANES), f32),
                pltpu.VMEM((LANES, LANES), f32),
                pltpu.VMEM((rows, ceil_to(side * rows, LANES)), f32),
                pltpu.VMEM((ceil_to(side * rows, LANES), width), f32),
                pltpu.VMEM((n, block * tiles * local, LANES), f32),
                pltpu.VMEM((n, block * tiles * local, LANES), f32),
                pltpu.VMEM((share, part_lanes), f32),
                pltpu.VMEM((n, share, part_lanes), f32),
                pltpu.SemaphoreType.DMA((7,)),
                dma,
                dma,
                dma,
                dma,
            ],
            compiler_params=pltpu.CompilerParams(
                collective_id=0, has_side_effects=True, vmem_limit_bytes=VMEM_GRANT
            ),
        )(
            *(
                pltpu.with_memory_space_constraint(value, pltpu.HBM)
                for value in (
                    images,
                    reference_image,
                    flat_kernels,
                    kernel_index,
                    flat_mask,
                    systematics,
                    onsets,
                )
            )
        )
        return pl.pallas_call(
            functools.partial(fit_kernel, float(rows * width)),
            out_shape=(
                jax.ShapeDtypeStruct((columns, block, width), f32),
                jax.ShapeDtypeStruct((epochs,), f32),
            ),
            in_specs=[vmem, vmem, vmem],
            out_specs=(vmem, vmem),
            scratch_shapes=[pltpu.VMEM((epochs, system_lanes), f32)],
            compiler_params=pltpu.CompilerParams(vmem_limit_bytes=VMEM_GRANT),
        )(pixels, total, base)

    in_specs = (
        P(("field", "ep"), None, None),
        P("field", None),
        P(),
        P(("field", "ep")),
        P(("field", "ep"), None, None),
        P("field", None),
        P("field"),
    )
    out_specs = (P(None, ("field", "ep"), None), P("field"))
    return jax.shard_map(shards, mesh=mesh, in_specs=in_specs, out_specs=out_specs, check_vma=False)
```
